256 devices in a mesh: dp: 64 (over x, z, core), mp: 4 (over y).
Axes of the slice: x: 4, y: 4, z: 8, core: 2. Of those that a mesh axis runs over, the one named last changes fastest.
Arguments:
- gradients: bfloat16 [32, 2048, 4096], P(None, 'dp', 'mp'), may hold values from -6 to 6
- statistics: float32 [65536, 4096], P('dp', 'mp'), may hold values from -3 to 3300, as said below
- row_counts: int32 [64], replicated, may hold values from 1 to 32, 1024 in all
- block_pair: int32 [32], replicated, may hold values from 0 to 31, each once
Outputs:
- update: bfloat16 [32, 2048, 4096], P(None, 'dp', 'mp')
- new_statistics: float32 [65536, 4096], P('dp', 'mp')
The draws below stay inside these ranges and needn't reach their ends.
Inputs may be any that keep to these rules, and one draw needn't show every extreme that they name: `row_counts`: the counts sum to 1024; the largest is exactly 32. `block_pair`: every pair index appears exactly once. `statistics`: each 1024 x 1024 block held by one device is symmetric positive definite.
All inputs are finite; a program needn't handle non-finite values. Where the reference program divides by a largest or mean magnitude, that divisor is 1e-20 or more.
Results may differ from the reference program's by a relative error of at most 0.0078.
The reference program's roundings to bfloat16 on the way count: a program that leaves them out, or rounds other values in their place, can miss the bound.
Values may be sent and summed in bfloat16 or wider, within the bound.
A program may use at most 64 MiB of HBM per device.

```python
import math
import jax
import jax.numpy as jnp
import numpy as np
from jax import lax

BLOCK = 1024
ITERS = 2
BLOCKS_MP = 32
MOST = 32
N_DP = 64
N_MP = 4


def draw_statistics(key, part):
    noise_key = jax.random.fold_in(key, 101)
    level_key = jax.random.fold_in(key, 202)
    row_key = jax.random.fold_in(key, 303)
    noise = jax.random.uniform(noise_key, (N_DP, N_MP, BLOCK, BLOCK), jnp.float32, -1.0, 1.0)
    symmetric = 0.5 * (noise + jnp.swapaxes(noise, 2, 3))
    level = jnp.exp(jax.random.uniform(level_key, (N_DP, N_MP), jnp.float32, jnp.log(10.0), jnp.log(100.0)))
    spread = jnp.exp(jax.random.uniform(row_key, (N_DP, N_MP, BLOCK), jnp.float32, 0.0, jnp.log(10.0)))
    diagonal = level[:, :, None] * spread
    root_diag = jnp.sqrt(diagonal)
    identity = jnp.eye(BLOCK, dtype=jnp.float32)
    matrix = root_diag[:, :, :, None] * root_diag[:, :, None, :] * (identity + 0.8 / (BLOCK - 1) * symmetric)
    return matrix.transpose(0, 2, 1, 3).reshape(N_DP * BLOCK, N_MP * BLOCK).astype(jnp.float32)


def level_of(stream_key, dims, split, low, largest):
    factor_of, own = 1.0, jax.random.fold_in(stream_key, 6)
    for dim, blocks in split:
        steps = jnp.exp(jax.random.uniform(jax.random.fold_in(own, dim), (blocks,), jnp.float32, low / len(split), largest / len(split)))
        factor_of = factor_of * jnp.repeat(steps, dims[dim] // blocks).reshape([-1 if axis == dim else 1 for axis in range(len(dims))])
    return factor_of


def length_profile(amount, total, most, lean):
    weights = [(1 << 20) // math.isqrt(standing ** lean) + 1 for standing in range(2, amount + 1)]
    surplus, given = total - most - (amount - 1), [1] * (amount - 1)
    while surplus > 0:
        movable = [i for i in range(amount - 1) if given[i] < most]
        pool, left = sum([weights[i] for i in movable]), surplus
        for i in movable:
            extra = min(most - given[i], max(1, left * weights[i] // pool), surplus)
            given[i] = given[i] + extra
            surplus = surplus - extra
    return np.array([most] + given)


def ragged(rng, amount, total, limit, lean):
    if amount == 2:
        one = jax.random.randint(rng, (), max(1, total - limit), min(limit, total - 1) + 1)
        return jnp.stack([one, total - one])
    lengths = jnp.asarray(length_profile(amount, total, limit, lean), jnp.int32)
    pairs = (amount - 1) // 2
    source_of, taker = lengths[1:1 + 2 * pairs:2], lengths[2:2 + 2 * pairs:2]
    margin = jnp.minimum(source_of - 1, limit - taker)
    moved = jax.random.randint(jax.random.fold_in(rng, 1), (pairs,), 0, 1 << 20) % (margin + 1)
    lengths = lengths.at[1:1 + 2 * pairs:2].set(source_of - moved).at[2:2 + 2 * pairs:2].set(taker + moved)
    return lengths[jax.random.permutation(jax.random.fold_in(rng, 2), amount)]


def scatter_about(stream_key, dims, scale, limit, split=(), kind=jnp.bfloat16):
    values = jax.random.normal(stream_key, dims, jnp.float32) * scale
    if len(split) > 0:
        values = level_of(stream_key, dims, split, -0.22, 0.18) * values
    return jnp.clip(values, min=-limit, max=limit).astype(kind)


def setup_inputs(seed: int = 0) -> dict:
    key_of = jax.random.split(jax.random.key(seed), 5)
    return {
        "gradients": scatter_about(key_of[0], (BLOCKS_MP, N_DP * MOST, N_MP * BLOCK), 1.0, 6.0, ((1, 64), (2, 4))),
        "statistics": draw_statistics(jax.random.fold_in(key_of[4], 71), 0),
        "row_counts": ragged(key_of[2], N_DP, BLOCK, MOST, 2).astype(jnp.int32),
        "block_pair": jax.random.permutation(key_of[3], N_DP // 2).astype(jnp.int32),
    }


decay_rate = 0.95
epsilon = 1e-06

def inverse_root(accumulated):
    block_size = accumulated.shape[0]
    bound = jnp.max(lax.optimization_barrier(jnp.sum(jnp.abs(accumulated), axis=1)))
    identity = jnp.eye(block_size, dtype=jnp.float32)
    moment = accumulated / bound
    factor = bound ** (-0.25)
    inv_root = None
    for iteration in range(ITERS):
        shifted = (5.0 * identity - moment) * 0.25
        poly_step = shifted.astype(jnp.bfloat16)
        if iteration == 0:
            inv_root = (factor * shifted).astype(jnp.bfloat16)
        else:
            inv_root = jnp.dot(inv_root, poly_step, preferred_element_type=jnp.float32).astype(jnp.bfloat16)
        if iteration + 1 < ITERS:
            square = jnp.dot(poly_step, poly_step, preferred_element_type=jnp.float32).astype(jnp.bfloat16)
            fourth = jnp.dot(square, square, preferred_element_type=jnp.float32).astype(jnp.bfloat16)
            moment = jnp.dot(fourth, moment.astype(jnp.bfloat16), preferred_element_type=jnp.float32)
    return inv_root

def reference(gradients, statistics, row_counts, block_pair):
    offsets = (jnp.cumsum(row_counts) - row_counts).astype(jnp.int32)
    row_ids = jnp.arange(BLOCK, dtype=jnp.int32)
    source = (lax.optimization_barrier(jnp.sum((offsets[None, :] <= row_ids[:, None]).astype(jnp.int32), axis=1)) - 1).astype(jnp.int32)
    gather_rows = (source * MOST + row_ids - jnp.take(offsets, source)).astype(jnp.int32)

    def one_block(flat_index):
        column = flat_index // BLOCKS_MP
        block_index = flat_index % BLOCKS_MP
        slab = lax.dynamic_index_in_dim(gradients, block_index, 0, keepdims=False)
        slab = lax.dynamic_slice_in_dim(slab, (column * BLOCK).astype(jnp.int32), BLOCK, 1)
        block_grad = jnp.take(slab, gather_rows, axis=0)
        left_owner = (2 * block_pair[block_index]).astype(jnp.int32)
        col_start = (column * BLOCK).astype(jnp.int32)
        left_prior = lax.dynamic_slice(statistics, ((left_owner * BLOCK).astype(jnp.int32), col_start), (BLOCK, BLOCK))
        right_prior = lax.dynamic_slice(statistics, (((left_owner + 1) * BLOCK).astype(jnp.int32), col_start), (BLOCK, BLOCK))
        left_stat = decay_rate * left_prior + (1.0 - decay_rate) * jnp.dot(block_grad, block_grad.T, preferred_element_type=jnp.float32)
        right_stat = decay_rate * right_prior + (1.0 - decay_rate) * jnp.dot(block_grad.T, block_grad, preferred_element_type=jnp.float32)
        left_root = inverse_root(left_stat)
        right_root = inverse_root(right_stat)
        half_prod = jnp.dot(left_root, block_grad, preferred_element_type=jnp.float32).astype(jnp.bfloat16)
        direction = jnp.dot(half_prod, right_root, preferred_element_type=jnp.float32)
        return (left_stat, right_stat, direction)
    left_all, right_all, directions = lax.map(one_block, jnp.arange(N_MP * BLOCKS_MP, dtype=jnp.int32))
    inv_rms = lax.rsqrt(jnp.mean(directions * directions) + epsilon)
    scaled = (directions * inv_rms).astype(jnp.bfloat16).reshape(N_MP, BLOCKS_MP, BLOCK, BLOCK)
    slot_ids = jnp.arange(MOST, dtype=jnp.int32)
    targets = offsets[:, None] + slot_ids[None, :]
    valid = slot_ids[None, :] < row_counts[:, None]
    picked = jnp.take(scaled, jnp.clip(targets, 0, BLOCK - 1).reshape(-1), axis=2)
    picked = jnp.where(valid.reshape(1, 1, -1, 1), picked, jnp.zeros((), jnp.bfloat16))
    update = picked.transpose(1, 2, 0, 3).reshape(BLOCKS_MP, N_DP * MOST, N_MP * BLOCK)
    pair_ids = jnp.arange(N_DP // 2, dtype=jnp.int32)
    block_ids = jnp.arange(BLOCKS_MP, dtype=jnp.int32)
    block_of_pair = lax.optimization_barrier(jnp.sum(block_ids[None, :] * (block_pair[None, :] == pair_ids[:, None]).astype(jnp.int32), axis=1)).astype(jnp.int32)
    device_ids = jnp.arange(N_DP, dtype=jnp.int32)
    device_block = jnp.take(block_of_pair, device_ids // 2)
    device_side = device_ids % 2
    stacked = jnp.stack([left_all.reshape(N_MP, BLOCKS_MP, BLOCK, BLOCK), right_all.reshape(N_MP, BLOCKS_MP, BLOCK, BLOCK)], axis=2)
    chosen = stacked[:, device_block, device_side]
    new_statistics = chosen.transpose(1, 2, 0, 3).reshape(N_DP * BLOCK, N_MP * BLOCK)
    return (update, new_statistics)
```

```python
import functools

import jax
import jax.numpy as jnp
from jax import lax
from jax.experimental import pallas as pl
from jax.experimental.pallas import tpu as pltpu
from jax.sharding import Mesh
from jax.sharding import PartitionSpec as P

DP = ("dp_0", "dp_1", "dp_2")
BLK = 1024
TILE = 256
F32 = jnp.float32
BF16 = jnp.bfloat16

decay_rate = 0.95
epsilon = 1e-06


def place():
    return (
        lax.axis_index("dp_0"),
        lax.axis_index("dp_1"),
        lax.axis_index("dp_2"),
        lax.axis_index("mp"),
    )


def distance(step):
    odd = step % 2
    return (4 + odd * ((step + 1) // 2) - (1 - odd) * (step // 2)) % 8


def dot(a, b, dims=((1,), (0,))):
    return lax.dot_general(a, b, (dims, ((), ())), preferred_element_type=F32)


def greet(peers):
    barrier = pltpu.get_barrier_semaphore()
    for peer in peers:
        pl.semaphore_signal(barrier, inc=1, device_id=peer)
    return barrier, len(peers)


def block_peers(x, z, c):
    peers = []
    for dx in range(4):
        for dz in range(8):
            for dc in range(2):
                if dx or dz or dc:
                    peers.append(
                        {"dp_0": (x + dx) % 4, "dp_1": (z + dz) % 8, "dp_2": (c + dc) % 2}
                    )
    return peers


def drain(ref, send_sem, recv_sem, c):
    return pltpu.make_async_remote_copy(
        ref, ref, send_sem, recv_sem, device_id={"dp_2": (c + 1) % 2}
    )


def forward_kernel(
    o_ref, t_ref, g_ref, recv, acc, send_sem, recv_sem, psend_sem, precv_sem, loc_sem
):
    x, z, c, _ = place()
    barrier, count = greet(block_peers(x, z, c))
    acc[...] = jnp.zeros_like(acc)
    pl.semaphore_wait(barrier, count)
    mine = 16 * (2 * x + c)

    def send_one(step, dist, dx, dc):
        tx, tz, tc = (x + dx) % 4, (z + dist) % 8, (c + dc) % 2
        pltpu.make_async_remote_copy(
            o_ref.at[tx * 8 + tz, pl.ds(pl.multiple_of(16 * tc, 16), 16), :],
            recv.at[step, pl.ds(pl.multiple_of(mine, 16), 16), :],
            send_sem.at[step],
            recv_sem.at[step],
            device_id={"dp_0": tx, "dp_1": tz, "dp_2": tc},
        ).start()

    @pl.loop(0, 7)
    def _(step):
        for dx in range(4):
            for dc in range(2):
                send_one(step, distance(step), dx, dc)

    for dx in range(4):
        for dc in range(2):
            if dx or dc:
                send_one(7, 0, dx, dc)
    own = pltpu.make_async_copy(
        o_ref.at[x * 8 + z, pl.ds(pl.multiple_of(16 * c, 16), 16), :],
        recv.at[7, pl.ds(pl.multiple_of(mine, 16), 16), :],
        loc_sem,
    )
    own.start()

    def to_partner(step):
        return pltpu.make_async_remote_copy(
            recv.at[step, pl.ds(0, 128), :],
            recv.at[step, pl.ds(128, 128), :],
            psend_sem.at[step],
            precv_sem.at[step],
            device_id={"dp_2": (c + 1) % 2},
        )

    rows = lax.broadcasted_iota(jnp.int32, (TILE, 128), 0)

    def put(step):
        to_partner(step).wait_recv()
        zs = (z + 8 - distance(step)) % 8
        near = t_ref[pl.ds(zs * 2 + c, 1), :]
        far = t_ref[pl.ds(zs * 2 + (c + 1) % 2, 1), :]
        chunk = recv[step]

        @pl.loop(0, BLK // TILE)
        def _(tile):
            at = rows + tile * TILE
            pick = jnp.concatenate([at == near, at == far], axis=1)
            pick = jnp.where(pick, 1.0, 0.0).astype(BF16)
            here = pl.ds(pl.multiple_of(tile * TILE, TILE), TILE)
            acc[here, :] += dot(pick, chunk)

    def take(step, rows_in):
        drain(recv.at[step, pl.ds(0, rows_in), :], send_sem.at[step], recv_sem.at[step], c).wait_recv()

    take(0, 128)
    to_partner(0).start()

    @pl.loop(1, 7)
    def _(step):
        take(step, 128)
        to_partner(step).start()
        put(step - 1)

    take(7, 112)
    own.wait()
    to_partner(7).start()
    put(6)
    put(7)

    @pl.loop(0, BLK // TILE)
    def _(tile):
        here = pl.ds(pl.multiple_of(tile * TILE, TILE), TILE)
        g_ref[here, :] = acc[here, :].astype(BF16)

    @pl.loop(0, 8)
    def _(step):
        to_partner(step).wait_send()

    @pl.loop(0, 7)
    def _(step):
        drain(recv.at[step, pl.ds(0, 128), :], send_sem.at[step], recv_sem.at[step], c).wait_send()

    drain(recv.at[7, pl.ds(0, 112), :], send_sem.at[7], recv_sem.at[7], c).wait_send()


def root_kernel(
    g_ref, s_ref, a_out, root_ref, a, poly, root, moment, work, fourth, in_sem, out_sem
):
    c = lax.axis_index("dp_2")
    tiles = BLK // TILE

    def span(tile):
        return pl.ds(pl.multiple_of(tile * TILE, TILE), TILE)

    def fetch(tile):
        return pltpu.make_async_copy(s_ref.at[span(tile), :], a.at[span(tile), :], in_sem.at[tile])

    def flush(tile):
        return pltpu.make_async_copy(a.at[span(tile), :], a_out.at[span(tile), :], out_sem.at[tile])

    for tile in range(tiles):
        fetch(tile).start()

    def gram(side):
        def step(tile, total):
            if side == 0:
                prod = dot(g_ref[span(tile), :], g_ref[...], ((1,), (1,)))
            else:
                prod = dot(g_ref[:, span(tile)], g_ref[...], ((0,), (0,)))
            fetch(tile).wait()
            new = decay_rate * a[span(tile), :] + (1.0 - decay_rate) * prod
            a[span(tile), :] = new
            return total + jnp.sum(jnp.abs(new).reshape(TILE // 8, 8, BLK), axis=0)

        total = lax.fori_loop(0, tiles, step, jnp.zeros((8, BLK), F32))
        work[pl.ds(0, 8), :] = total

    pl.when(c == 0)(lambda: gram(0))
    pl.when(c == 1)(lambda: gram(1))
    for tile in range(tiles):
        flush(tile).start()
    bound = jnp.max(jnp.sum(work[pl.ds(0, 8), :], axis=0, keepdims=True), axis=1, keepdims=True)
    scale = 1.0 / bound
    factor = lax.rsqrt(jnp.sqrt(bound))
    row = lax.broadcasted_iota(jnp.int32, (TILE, BLK), 0)
    col = lax.broadcasted_iota(jnp.int32, (TILE, BLK), 1)

    def eye5(tile):
        return jnp.where(row + tile * TILE == col, 5.0, 0.0)

    @pl.loop(0, tiles)
    def _(tile):
        first = a[span(tile), :] * scale
        shifted = (eye5(tile) - first) * 0.25
        moment[span(tile), :] = first.astype(BF16)
        poly[span(tile), :] = shifted.astype(BF16)
        root[span(tile), :] = (factor * shifted).astype(BF16)

    work16 = fourth.at[0]
    four = fourth.at[1]

    @pl.loop(0, tiles)
    def _(tile):
        work16[span(tile), :] = dot(poly[span(tile), :], poly[...]).astype(BF16)

    @pl.loop(0, tiles)
    def _(tile):
        four[span(tile), :] = dot(work16[span(tile), :], work16[...]).astype(BF16)

    @pl.loop(0, tiles)
    def _(tile):
        new = dot(four[span(tile), :], moment[...])
        poly[span(tile), :] = ((eye5(tile) - new) * 0.25).astype(BF16)

    @pl.loop(0, tiles)
    def _(tile):
        root_ref[span(tile), :] = dot(root[span(tile), :], poly[...]).astype(BF16)

    for tile in range(tiles):
        flush(tile).wait()


def backward_kernel(
    entries,
    root_ref,
    g_ref,
    t_ref,
    f_ref,
    scale_ref,
    roots,
    ways,
    square,
    small,
    ring,
    loc_sem,
    root_sem,
    send_sem,
    recv_sem,
    near_sem,
    sum_send,
    sum_recv,
):
    x, z, c, y = place()
    partner = {"dp_2": (c + 1) % 2}
    peers = block_peers(x, z, c) + [{"mp": (y + dy) % 4} for dy in range(1, 4)]
    barrier, count = greet(peers)
    keep = pltpu.make_async_copy(root_ref, roots.at[c], loc_sem.at[0])
    keep.start()
    square[...] = jnp.zeros_like(square)
    pl.semaphore_wait(barrier, count)
    swap = pltpu.make_async_remote_copy(
        root_ref, roots.at[c], root_sem.at[0], root_sem.at[1], device_id=partner
    )
    swap.start()
    keep.wait()
    swap.wait_recv()
    cols = lax.broadcasted_iota(jnp.int32, (128, BLK), 1).astype(F32)

    def wanted(step):
        zt = (z + distance(step)) % 8
        line = t_ref[pl.ds(zt * 2 + c, 1), :].astype(F32)
        turned = jnp.transpose(jnp.broadcast_to(line, (128, 128)))
        return jnp.where(jnp.concatenate([turned] * 8, axis=1) == cols, 1.0, 0.0).astype(BF16)

    def make(pair):
        pick = jnp.concatenate([wanted(2 * pair), wanted(2 * pair + 1)], axis=0)
        picked = dot(pick, roots[0]).astype(BF16)
        half = dot(picked, g_ref[...]).astype(BF16)
        full = dot(half, roots[1])
        ways[pl.ds(pl.multiple_of(pair * 256, 256), 256), :] = full.astype(BF16)
        square[...] += jnp.sum((full * full).reshape(32, 8, BLK), axis=0)

    slot = pl.ds(pl.multiple_of(16 * c, 16), 16)

    def send_one(step, dist, dx, dc, ssem, rsem):
        tx, tz, tc = (x + dx) % 4, (z + dist) % 8, (c + dc) % 2
        return pltpu.make_async_remote_copy(
            ways.at[pl.ds(pl.multiple_of(step * 128 + 16 * (2 * tx + tc), 16), 16), :],
            f_ref.at[x * 8 + z, slot, :],
            ssem,
            rsem,
            device_id={"dp_0": tx, "dp_1": tz, "dp_2": tc},
        )

    def send_step(step):
        for dx in range(4):
            for dc in range(2):
                send_one(step, distance(step), dx, dc, send_sem, recv_sem).start()

    @pl.loop(0, 2)
    def _(pair):
        make(pair)
        send_step(2 * pair)
        send_step(2 * pair + 1)

    @pl.loop(2, 4)
    def _(pair):
        make(pair)

    own = jnp.sum(square[...], axis=0, keepdims=True)
    part = own[:, 0:128]
    for i in range(1, 8):
        part = part + own[:, 128 * i : 128 * (i + 1)]
    one = pl.ds(0, 1)
    small[0, one, :] = part
    pair_sum = pltpu.make_async_remote_copy(
        small.at[0, one, :], small.at[3, one, :], sum_send.at[0], sum_recv.at[0], device_id=partner
    )
    pair_sum.start()
    pair_sum.wait_recv()
    part = part + small[3, one, :]
    small[1, one, :] = part
    for dy in range(1, 4):
        pltpu.make_async_remote_copy(
            small.at[1, one, :],
            small.at[3 + dy, one, :],
            sum_send.at[1],
            sum_recv.at[1],
            device_id={"mp": (y + dy) % 4},
        ).start()
    three = pltpu.make_async_remote_copy(
        small.at[pl.ds(4, 3), one, :],
        small.at[pl.ds(4, 3), one, :],
        sum_send.at[1],
        sum_recv.at[1],
        device_id={"mp": (y + 1) % 4},
    )
    three.wait_recv()
    for dy in range(1, 4):
        part = part + small[3 + dy, one, :]
    small[2, one, :] = part
    for dx in range(4):
        for dz in range(8):
            if dx or dz:
                pltpu.make_async_remote_copy(
                    small.at[2, one, :],
                    ring.at[dx * 8 + dz - 1, one, :],
                    sum_send.at[2],
                    sum_recv.at[2],
                    device_id={"dp_0": (x + dx) % 4, "dp_1": (z + dz) % 8},
                ).start()

    send_step(4)
    send_step(5)
    send_step(6)
    last = []
    for dx in range(4):
        for dc in range(2):
            if dx == 0 and dc == 0:
                continue
            if dx == 0:
                last.append(send_one(7, 0, dx, dc, near_sem.at[0], near_sem.at[1]))
            else:
                last.append(send_one(7, 0, dx, dc, send_sem, recv_sem))
            last[-1].start()
    stay = pltpu.make_async_copy(
        ways.at[pl.ds(pl.multiple_of(7 * 128 + 16 * (2 * x + c), 16), 16), :],
        f_ref.at[x * 8 + z, slot, :],
        loc_sem.at[1],
    )
    stay.start()
    everyone = pltpu.make_async_remote_copy(
        ring.at[pl.ds(0, 31), one, :],
        ring.at[pl.ds(0, 31), one, :],
        sum_send.at[2],
        sum_recv.at[2],
        device_id=partner,
    )
    everyone.wait_recv()
    for i in range(31):
        part = part + ring[i, one, :]
    mean = jnp.sum(part, axis=1, keepdims=True) * (1.0 / entries)
    scale_ref[...] = jnp.broadcast_to(lax.rsqrt(mean + epsilon), (8, 128))

    swap.wait_send()
    pair_sum.wait_send()
    three.wait_send()
    everyone.wait_send()
    stay.wait()
    last[0].wait_send()
    last[0].wait_recv()
    bulk = pltpu.make_async_remote_copy(
        ways.at[pl.ds(0, 992), :], ways.at[pl.ds(0, 992), :], send_sem, recv_sem, device_id=partner
    )
    bulk.wait_send()
    bulk.wait_recv()


VMEM = pl.BlockSpec(memory_space=pltpu.VMEM)
ANY = pl.BlockSpec(memory_space=pl.ANY)
DMA = pltpu.SemaphoreType.DMA


def shape(dims, kind):
    return jax.ShapeDtypeStruct(dims, kind)


def body(gradients, statistics, row_counts, block_pair):
    blocks, slots, _ = gradients.shape
    devices = lax.axis_size(DP)
    ids = jnp.arange(devices // 2, dtype=jnp.int32)
    block_of = jnp.sum(jnp.where(block_pair[None, :] == ids[:, None], ids[None, :], 0), axis=1)
    outgoing = jnp.take(gradients, block_of, axis=0, mode="clip")
    peers = jnp.arange(devices, dtype=jnp.int32)
    before = peers[None, :] < peers[:, None]
    offsets = jnp.sum(jnp.where(before, row_counts[None, :], 0), axis=1)
    slot_ids = jnp.arange(slots, dtype=jnp.int32)
    table = jnp.where(
        slot_ids[None, :] < row_counts[:, None], offsets[:, None] + slot_ids[None, :], -1
    )
    table = table.reshape(4, 8, 2, 2, 16).transpose(1, 3, 0, 2, 4).reshape(16, 128)

    grad = pl.pallas_call(
        forward_kernel,
        out_shape=shape((BLK, BLK), BF16),
        in_specs=[ANY, VMEM],
        out_specs=VMEM,
        scratch_shapes=[
            pltpu.VMEM((8, 256, BLK), BF16),
            pltpu.VMEM((BLK, BLK), F32),
            DMA((8,)),
            DMA((8,)),
            DMA((8,)),
            DMA((8,)),
            DMA,
        ],
        compiler_params=pltpu.CompilerParams(
            collective_id=0, has_side_effects=True, vmem_limit_bytes=48 << 20
        ),
        name="forward",
    )(outgoing, table)

    accumulated, root = pl.pallas_call(
        root_kernel,
        out_shape=(shape((BLK, BLK), F32), shape((BLK, BLK), BF16)),
        in_specs=[VMEM, ANY],
        out_specs=(ANY, VMEM),
        scratch_shapes=[
            pltpu.VMEM((BLK, BLK), F32),
            pltpu.VMEM((BLK, BLK), BF16),
            pltpu.VMEM((BLK, BLK), BF16),
            pltpu.VMEM((BLK, BLK), BF16),
            pltpu.VMEM((8, BLK), F32),
            pltpu.VMEM((2, BLK, BLK), BF16),
            DMA((4,)),
            DMA((4,)),
        ],
        compiler_params=pltpu.CompilerParams(vmem_limit_bytes=48 << 20),
        name="roots",
    )(grad, statistics)

    entries = lax.axis_size("mp") * blocks * BLK * BLK
    returned, scale = pl.pallas_call(
        functools.partial(backward_kernel, entries),
        out_shape=(shape((blocks, slots, BLK), BF16), shape((8, 128), F32)),
        in_specs=[ANY, VMEM, VMEM],
        out_specs=(ANY, VMEM),
        scratch_shapes=[
            pltpu.VMEM((2, BLK, BLK), BF16),
            pltpu.VMEM((BLK, BLK), BF16),
            pltpu.VMEM((8, BLK), F32),
            pltpu.VMEM((8, 8, 128), F32),
            pltpu.VMEM((32, 8, 128), F32),
            DMA((2,)),
            DMA((2,)),
            DMA,
            DMA,
            DMA((2,)),
            DMA((3,)),
            DMA((3,)),
        ],
        compiler_params=pltpu.CompilerParams(
            collective_id=1, has_side_effects=True, vmem_limit_bytes=48 << 20
        ),
        name="backward",
    )(root, grad, table)

    update = (jnp.take(returned, block_pair, axis=0, mode="clip").astype(F32) * scale[0, 0]).astype(BF16)
    return (update, accumulated)


def solution(mesh):
    torus = Mesh(mesh.devices.reshape(4, 8, 2, mesh.shape["mp"]), DP + ("mp",))
    placed = (P(None, DP, "mp"), P(DP, "mp"), P(), P())
    return jax.shard_map(
        body,
        mesh=torus,
        in_specs=placed,
        out_specs=(P(None, DP, "mp"), P(DP, "mp")),
        check_vma=False,
    )
```

```python
import functools

import jax
import jax.numpy as jnp
from jax import lax
from jax.experimental import pallas as pl
from jax.experimental.pallas import tpu as pltpu
from jax.sharding import Mesh
from jax.sharding import PartitionSpec as P

DP = ("dp_0", "dp_1", "dp_2")
BLK = 1024
TILE = 256
F32 = jnp.float32
BF16 = jnp.bfloat16

decay_rate = 0.95
epsilon = 1e-06


def place():
    return (
        lax.axis_index("dp_0"),
        lax.axis_index("dp_1"),
        lax.axis_index("dp_2"),
        lax.axis_index("mp"),
    )


def distance(step):
    odd = step % 2
    return (4 + odd * ((step + 1) // 2) - (1 - odd) * (step // 2)) % 8


def dot(a, b, dims=((1,), (0,))):
    return lax.dot_general(a, b, (dims, ((), ())), preferred_element_type=F32)


def greet(peers):
    barrier = pltpu.get_barrier_semaphore()
    for peer in peers:
        pl.semaphore_signal(barrier, inc=1, device_id=peer)
    return barrier, len(peers)


def plane_peers(x, c):
    return [
        {"dp_0": (x + dx) % 4, "dp_2": (c + dc) % 2}
        for dx in range(4)
        for dc in range(2)
        if dx or dc
    ]


def z_peers(z):
    return [{"dp_1": (z + dz) % 8} for dz in range(1, 8)]


def transfer(ref, send_sem, recv_sem, c):
    return pltpu.make_async_remote_copy(
        ref, ref, send_sem, recv_sem, device_id={"dp_2": (c + 1) % 2}
    )


def half_of(c):
    return pl.ds(pl.multiple_of(512 * c, 512), 512)


def slots_of(x, c):
    return pl.ds(pl.multiple_of(32 * (2 * x + c), 32), 32)


def span(tile):
    return pl.ds(pl.multiple_of(tile * TILE, TILE), TILE)


def deal_kernel(counts, pair, g_ref, o_ref, t_ref):
    @pl.loop(0, 32)
    def _(k):
        o_ref[pair[k]] = g_ref[k]

    lane = lax.broadcasted_iota(jnp.int32, (8, 256), 1)
    plane = lax.broadcasted_iota(jnp.int32, (8, 256), 0)
    inner = lane % 32
    group = lane // 32
    spot = jnp.full((8, 256), -1, jnp.int32)
    target = jnp.full((8, 256), -1, jnp.int32)
    offset = counts[0] * 0
    filled = [offset] * 8
    for x in range(4):
        for z in range(8):
            for c in range(2):
                q = (x * 8 + z) * 2 + c
                n = counts[q]
                at = filled[z]
                here = (plane == z) & (group == 2 * x + c) & (inner < n)
                spot = jnp.where(here, at + inner, spot)
                held = (plane == z) & (lane >= at) & (lane < at + n)
                target = jnp.where(held, offset - at + lane, target)
                filled[z] = at + n
                offset = offset + n
    t_ref[0:8, :] = spot
    t_ref[8:16, :] = target


def forward_kernel(
    room,
    o_ref,
    t_ref,
    g_ref,
    near,
    packed,
    recv,
    acc,
    pick_ref,
    x_send,
    x_recv,
    z_send,
    z_recv,
    p_send,
    p_recv,
):
    x, z, c, _ = place()
    barrier, count = greet(plane_peers(x, c) + z_peers(z))
    spot = t_ref[pl.ds(z, 1), :]
    rows = lax.broadcasted_iota(jnp.int32, (256, 256), 0)
    pick_ref[...] = jnp.where(rows == spot, 1.0, 0.0).astype(BF16)
    pl.semaphore_wait(barrier, count)

    def give(step):
        tz = (z + distance(step)) % 8
        for dx in range(4):
            for dc in range(2):
                tx, tc = (x + dx) % 4, (c + dc) % 2
                if dx or dc:
                    pltpu.make_async_remote_copy(
                        o_ref.at[tx * 8 + tz, :, half_of(tc)],
                        near.at[step, slots_of(x, c), :],
                        x_send,
                        x_recv.at[step],
                        device_id={"dp_0": tx, "dp_2": tc},
                    ).start()

    @pl.loop(0, 8)
    def _(step):
        give(step)

    def keep(step):
        tz = (z + distance(step)) % 8
        near[step, slots_of(x, c), :] = o_ref[x * 8 + tz, :, half_of(c)]

    @pl.loop(0, 8)
    def _(step):
        keep(step)

    def pack(step):
        transfer(near.at[step, pl.ds(0, 224), :], x_send, x_recv.at[step], c).wait_recv()
        return dot(pick_ref[pl.ds(0, room), :], near[step]).astype(BF16)

    def to_partner(step):
        part = recv.at[step, :, half_of(c)]
        return pltpu.make_async_remote_copy(
            part, part, p_send.at[step], p_recv.at[step], device_id={"dp_2": (c + 1) % 2}
        )

    @pl.loop(0, 7)
    def _(step):
        packed[step] = pack(step)
        pltpu.make_async_remote_copy(
            packed.at[step],
            recv.at[step, :, half_of(c)],
            z_send,
            z_recv.at[step],
            device_id={"dp_1": (z + distance(step)) % 8},
        ).start()

    recv[7, :, half_of(c)] = pack(7)
    to_partner(7).start()
    lines = lax.broadcasted_iota(jnp.int32, (TILE, room), 0)

    def put(step, first=False, last=False):
        to_partner(step).wait_recv()
        zs = (z + 8 - distance(step)) % 8
        target = t_ref[pl.ds(8 + zs, 1), :][:, 0:room]

        @pl.loop(0, BLK // TILE)
        def _(tile):
            pick = jnp.where(lines + tile * TILE == target, 1.0, 0.0).astype(BF16)
            new = dot(pick, recv[step])
            if not first:
                new = acc[span(tile), :] + new
            if last:
                g_ref[span(tile), :] = new.astype(BF16)
            else:
                acc[span(tile), :] = new

    def take(step):
        transfer(packed.at[step], z_send, z_recv.at[step], c).wait_recv()
        to_partner(step).start()

    take(0)
    put(7, first=True)

    @pl.loop(1, 7)
    def _(step):
        take(step)
        put(step - 1)

    put(6, last=True)

    @pl.loop(0, 8)
    def _(step):
        to_partner(step).wait_send()

    transfer(near.at[pl.ds(0, 7)], x_send, x_recv.at[0], c).wait_send()
    transfer(packed, z_send, z_recv.at[0], c).wait_send()


def root_kernel(
    g_ref, s_ref, a_out, root, step_ref, a, poly, moment, work, fourth, in_sem, out_sem
):
    c = lax.axis_index("dp_2")
    tiles = BLK // TILE

    def fetch(tile):
        return pltpu.make_async_copy(s_ref.at[span(tile), :], a.at[span(tile), :], in_sem.at[tile])

    def flush(tile):
        return pltpu.make_async_copy(a.at[span(tile), :], a_out.at[span(tile), :], out_sem.at[tile])

    for tile in range(tiles):
        fetch(tile).start()

    def gram(side):
        def step(tile, total):
            if side == 0:
                prod = dot(g_ref[span(tile), :], g_ref[...], ((1,), (1,)))
            else:
                prod = dot(g_ref[:, span(tile)], g_ref[...], ((0,), (0,)))
            fetch(tile).wait()
            new = decay_rate * a[span(tile), :] + (1.0 - decay_rate) * prod
            a[span(tile), :] = new
            return total + jnp.sum(jnp.abs(new).reshape(TILE // 8, 8, BLK), axis=0)

        total = lax.fori_loop(0, tiles, step, jnp.zeros((8, BLK), F32))
        work[pl.ds(0, 8), :] = total

    pl.when(c == 0)(lambda: gram(0))
    pl.when(c == 1)(lambda: gram(1))
    for tile in range(tiles):
        flush(tile).start()
    bound = jnp.max(jnp.sum(work[pl.ds(0, 8), :], axis=0, keepdims=True), axis=1, keepdims=True)
    scale = 1.0 / bound
    factor = lax.rsqrt(jnp.sqrt(bound))
    row = lax.broadcasted_iota(jnp.int32, (TILE, BLK), 0)
    col = lax.broadcasted_iota(jnp.int32, (TILE, BLK), 1)

    def eye5(tile):
        return jnp.where(row + tile * TILE == col, 5.0, 0.0)

    @pl.loop(0, tiles)
    def _(tile):
        first = a[span(tile), :] * scale
        shifted = (eye5(tile) - first) * 0.25
        moment[span(tile), :] = first.astype(BF16)
        poly[span(tile), :] = shifted.astype(BF16)
        root[span(tile), :] = (factor * shifted).astype(BF16)

    work16 = fourth.at[0]
    four = fourth.at[1]

    @pl.loop(0, tiles)
    def _(tile):
        work16[span(tile), :] = dot(poly[span(tile), :], poly[...]).astype(BF16)

    @pl.loop(0, tiles)
    def _(tile):
        four[span(tile), :] = dot(work16[span(tile), :], work16[...]).astype(BF16)

    @pl.loop(0, tiles)
    def _(tile):
        new = dot(four[span(tile), :], moment[...])
        step_ref[span(tile), :] = ((eye5(tile) - new) * 0.25).astype(BF16)

    for tile in range(tiles):
        flush(tile).wait()


def backward_kernel(
    room,
    entries,
    root_ref,
    step_ref,
    g_ref,
    t_ref,
    f_ref,
    scale_ref,
    roots,
    ways,
    back,
    slots,
    spread_ref,
    square,
    told,
    heard,
    root_sem,
    z_send,
    z_recv,
    x_send,
    x_recv,
    sum_send,
    sum_recv,
):
    x, z, c, y = place()
    partner = {"dp_2": (c + 1) % 2}
    y_peers = [{"mp": (y + dy) % 4} for dy in range(1, 4)]
    x_peers = [{"dp_0": (x + dx) % 4} for dx in range(1, 4)]
    barrier, count = greet(plane_peers(x, c) + z_peers(z) + y_peers)

    def make_root(tile):
        roots[c, span(tile), :] = dot(root_ref[span(tile), :], step_ref[...]).astype(BF16)

    def swap(tile):
        part = roots.at[c, span(tile), :]
        return pltpu.make_async_remote_copy(
            part, part, root_sem.at[0], root_sem.at[1], device_id=partner
        )

    def column(line):
        turned = jnp.transpose(jnp.broadcast_to(line.astype(F32), (128, 256)))
        return jnp.concatenate([turned] * 8, axis=1)

    cols = lax.broadcasted_iota(jnp.int32, (256, BLK), 1).astype(F32)
    spread = jnp.where(column(t_ref[pl.ds(z, 1), :]) == cols, 1.0, 0.0)
    spread_ref[...] = spread[:, 0:256].astype(BF16)
    square[...] = jnp.zeros_like(square)

    @pl.loop(0, 2)
    def _(tile):
        make_root(tile)

    pl.semaphore_wait(barrier, count)
    swap(0).start()
    swap(1).start()

    @pl.loop(2, 4)
    def _(tile):
        make_root(tile)
        swap(tile).start()

    whole = transfer(roots.at[c], root_sem.at[0], root_sem.at[1], c)
    whole.wait_recv()

    def make(step):
        zt = (z + distance(step)) % 8
        want = column(t_ref[pl.ds(8 + zt, 1), :]) == cols
        pick = jnp.where(want, 1.0, 0.0).astype(BF16)[0:room, :]
        picked = dot(pick, roots[0]).astype(BF16)
        half = dot(picked, g_ref[...]).astype(BF16)
        full = dot(half, roots[1, :, half_of(c)])
        ways[step] = full.astype(BF16)
        square[...] += jnp.sum((full * full).reshape(room // 8, 8, 512), axis=0)

    @pl.loop(0, 7)
    def _(step):
        make(step)
        pltpu.make_async_remote_copy(
            ways.at[step],
            back.at[step],
            z_send,
            z_recv.at[step],
            device_id={"dp_1": (z + distance(step)) % 8},
        ).start()

    make(7)
    one = pl.ds(0, 1)

    def tell(stage, part, peers, at):
        told[stage, one, :] = part
        for i, peer in enumerate(peers):
            pltpu.make_async_remote_copy(
                told.at[stage, one, :],
                heard.at[at + i, one, :],
                sum_send.at[stage],
                sum_recv.at[stage],
                device_id=peer,
            ).start()

    def hear(stage, part, number, at):
        ref = heard.at[pl.ds(at, number), one, :]
        transfer(ref, sum_send.at[stage], sum_recv.at[stage], c).wait()
        for i in range(number):
            part = part + heard[at + i, one, :]
        return part

    def give(step, rows):
        slots[step] = dot(spread_ref[:, 0:room], rows).astype(BF16)
        block = x * 8 + (z + 8 - distance(step)) % 8
        for dx in range(4):
            for dc in range(2):
                tx, tc = (x + dx) % 4, (c + dc) % 2
                if dx or dc:
                    pltpu.make_async_remote_copy(
                        slots.at[step, slots_of(tx, tc), :],
                        f_ref.at[block, :, half_of(c)],
                        x_send,
                        x_recv,
                        device_id={"dp_0": tx, "dp_2": tc},
                    ).start()
        f_ref[block, :, half_of(c)] = slots[step, slots_of(x, c), :]

    def pass_on(step):
        transfer(back.at[step], z_send, z_recv.at[step], c).wait_recv()
        give(step, back[step])

    own = jnp.sum(square[...], axis=0, keepdims=True)
    part = own[:, 0:128] + own[:, 128:256] + own[:, 256:384] + own[:, 384:512]
    tell(0, part, [partner], 0)
    give(7, ways[7])
    part = hear(0, part, 1, 0)
    tell(1, part, y_peers, 1)
    pass_on(0)
    part = hear(1, part, 3, 1)
    tell(2, part, x_peers, 4)
    pass_on(1)
    part = hear(2, part, 3, 4)
    tell(3, part, z_peers(z), 7)

    @pl.loop(2, 7)
    def _(step):
        pass_on(step)

    part = hear(3, part, 7, 7)
    mean = jnp.sum(part, axis=1, keepdims=True) * (1.0 / entries)
    scale_ref[...] = jnp.broadcast_to(lax.rsqrt(mean + epsilon), (8, 128))
    whole.wait_send()
    transfer(ways.at[pl.ds(0, 7)], z_send, z_recv.at[0], c).wait_send()
    transfer(slots.at[pl.ds(0, 7)], x_send, x_recv, c).wait_send()
    transfer(f_ref.at[pl.ds(0, 28)], x_send, x_recv, c).wait_recv()


def finish_kernel(pair, scale_ref, f_ref, u_ref, held, sem):
    scale = scale_ref[0:1, 0:1]

    def flush(group):
        part = pl.ds(group * 8, 8)
        return pltpu.make_async_copy(held.at[part], u_ref.at[part], sem.at[group])

    @pl.loop(0, 4)
    def _(group):
        for i in range(8):
            k = group * 8 + i
            held[k] = (f_ref[pair[k]].astype(F32) * scale).astype(BF16)
        flush(group).start()

    for group in range(4):
        flush(group).wait()


VMEM = pl.BlockSpec(memory_space=pltpu.VMEM)
SMEM = pl.BlockSpec(memory_space=pltpu.SMEM)
ANY = pl.BlockSpec(memory_space=pl.ANY)
DMA = pltpu.SemaphoreType.DMA
LIMIT = 48 << 20
ROOM = 192
FULL = 256


def shape(dims, kind):
    return jax.ShapeDtypeStruct(dims, kind)


def remote(number):
    return pltpu.CompilerParams(
        collective_id=number, has_side_effects=True, vmem_limit_bytes=LIMIT
    )


def forward(room, number):
    return pl.pallas_call(
        functools.partial(forward_kernel, room),
        out_shape=shape((BLK, BLK), BF16),
        in_specs=[VMEM, VMEM],
        out_specs=VMEM,
        scratch_shapes=[
            pltpu.VMEM((8, 256, 512), BF16),
            pltpu.VMEM((7, room, 512), BF16),
            pltpu.VMEM((8, room, BLK), BF16),
            pltpu.VMEM((BLK, BLK), F32),
            pltpu.VMEM((256, 256), BF16),
            DMA,
            DMA((8,)),
            DMA,
            DMA((7,)),
            DMA((8,)),
            DMA((8,)),
        ],
        compiler_params=remote(number),
        name=f"forward_{room}",
    )


def backward(room, number, entries):
    return pl.pallas_call(
        functools.partial(backward_kernel, room, entries),
        out_shape=(shape((32, 32, BLK), BF16), shape((8, 128), F32)),
        in_specs=[VMEM] * 4,
        out_specs=(VMEM, VMEM),
        scratch_shapes=[
            pltpu.VMEM((2, BLK, BLK), BF16),
            pltpu.VMEM((8, room, 512), BF16),
            pltpu.VMEM((7, room, 512), BF16),
            pltpu.VMEM((8, 256, 512), BF16),
            pltpu.VMEM((256, 256), BF16),
            pltpu.VMEM((8, 512), F32),
            pltpu.VMEM((4, 8, 128), F32),
            pltpu.VMEM((16, 8, 128), F32),
            DMA((2,)),
            DMA,
            DMA((7,)),
            DMA,
            DMA,
            DMA((4,)),
            DMA((4,)),
        ],
        compiler_params=remote(number),
        name=f"backward_{room}",
    )


def body(gradients, statistics, row_counts, block_pair):
    blocks = gradients.shape[0]
    outgoing, table = pl.pallas_call(
        deal_kernel,
        out_shape=(shape(gradients.shape, BF16), shape((16, 256), jnp.int32)),
        in_specs=[SMEM, SMEM, VMEM],
        out_specs=(VMEM, VMEM),
        compiler_params=pltpu.CompilerParams(vmem_limit_bytes=16 << 20),
        name="deal",
    )(row_counts, block_pair, gradients)
    planes = jnp.sum(row_counts.reshape(4, 8, 2), axis=(0, 2))
    fits = jnp.max(planes) <= ROOM

    grad = lax.cond(fits, forward(ROOM, 0), forward(FULL, 1), outgoing, table)

    accumulated, root, step = pl.pallas_call(
        root_kernel,
        out_shape=(shape((BLK, BLK), F32), shape((BLK, BLK), BF16), shape((BLK, BLK), BF16)),
        in_specs=[VMEM, ANY],
        out_specs=(ANY, VMEM, VMEM),
        scratch_shapes=[
            pltpu.VMEM((BLK, BLK), F32),
            pltpu.VMEM((BLK, BLK), BF16),
            pltpu.VMEM((BLK, BLK), BF16),
            pltpu.VMEM((8, BLK), F32),
            pltpu.VMEM((2, BLK, BLK), BF16),
            DMA((4,)),
            DMA((4,)),
        ],
        compiler_params=pltpu.CompilerParams(vmem_limit_bytes=LIMIT),
        name="roots",
    )(grad, statistics)

    entries = lax.axis_size("mp") * blocks * BLK * BLK
    returned, scale = lax.cond(
        fits, backward(ROOM, 2, entries), backward(FULL, 3, entries), root, step, grad, table
    )

    update = pl.pallas_call(
        finish_kernel,
        out_shape=shape(gradients.shape, BF16),
        in_specs=[SMEM, VMEM, VMEM],
        out_specs=ANY,
        scratch_shapes=[pltpu.VMEM(gradients.shape, BF16), DMA((4,))],
        compiler_params=pltpu.CompilerParams(vmem_limit_bytes=16 << 20),
        name="finish",
    )(block_pair, scale, returned)
    return (update, accumulated)


def solution(mesh):
    torus = Mesh(mesh.devices.reshape(4, 8, 2, mesh.shape["mp"]), DP + ("mp",))
    placed = (P(None, DP, "mp"), P(DP, "mp"), P(), P())
    return jax.shard_map(
        body,
        mesh=torus,
        in_specs=placed,
        out_specs=(P(None, DP, "mp"), P(DP, "mp")),
        check_vma=False,
    )
```

```python
import functools

import jax
import jax.numpy as jnp
from jax import lax
from jax.experimental import pallas as pl
from jax.experimental.pallas import tpu as pltpu
from jax.sharding import Mesh
from jax.sharding import PartitionSpec as P

DP = ("dp_0", "dp_1", "dp_2")
BLK = 1024
TILE = 256
F32 = jnp.float32
BF16 = jnp.bfloat16

decay_rate = 0.95
epsilon = 1e-06


def place():
    return (
        lax.axis_index("dp_0"),
        lax.axis_index("dp_1"),
        lax.axis_index("dp_2"),
        lax.axis_index("mp"),
    )


def distance(step):
    odd = step % 2
    return (4 + odd * ((step + 1) // 2) - (1 - odd) * (step // 2)) % 8


def dot(a, b, dims=((1,), (0,))):
    return lax.dot_general(a, b, (dims, ((), ())), preferred_element_type=F32)


def greet(peers):
    barrier = pltpu.get_barrier_semaphore()
    for peer in peers:
        pl.semaphore_signal(barrier, inc=1, device_id=peer)
    return barrier, len(peers)


def plane_peers(x, c):
    return [
        {"dp_0": (x + dx) % 4, "dp_2": (c + dc) % 2}
        for dx in range(4)
        for dc in range(2)
        if dx or dc
    ]


def z_peers(z):
    return [{"dp_1": (z + dz) % 8} for dz in range(1, 8)]


def transfer(ref, send_sem, recv_sem, c):
    return pltpu.make_async_remote_copy(
        ref, ref, send_sem, recv_sem, device_id={"dp_2": (c + 1) % 2}
    )


def half_of(c):
    return pl.ds(pl.multiple_of(512 * c, 512), 512)


def slots_of(x, c):
    return pl.ds(pl.multiple_of(32 * (2 * x + c), 32), 32)


def span(tile):
    return pl.ds(pl.multiple_of(tile * TILE, TILE), TILE)


def deal_kernel(
    counts_ref, pair_ref, g_ref, o_ref, t_ref, level_ref, counts, pair, sem, block_sem
):
    first = pltpu.make_async_copy(pair_ref, pair, sem.at[0])
    second = pltpu.make_async_copy(counts_ref, counts, sem.at[1])
    first.start()
    second.start()
    first.wait()

    @pl.loop(0, 32)
    def _(k):
        pltpu.make_async_copy(g_ref.at[k], o_ref.at[pair[k]], block_sem).start()

    second.wait()
    lane = lax.broadcasted_iota(jnp.int32, (8, 256), 1)
    plane = lax.broadcasted_iota(jnp.int32, (8, 256), 0)
    inner = lane % 32
    group = lane // 32
    spot = jnp.full((8, 256), -1, jnp.int32)
    target = jnp.full((8, 256), -1, jnp.int32)
    offset = counts[0] * 0
    filled = [offset] * 8
    for x in range(4):
        for z in range(8):
            for c in range(2):
                q = (x * 8 + z) * 2 + c
                n = counts[q]
                at = filled[z]
                here = (plane == z) & (group == 2 * x + c) & (inner < n)
                spot = jnp.where(here, at + inner, spot)
                held = (plane == z) & (lane >= at) & (lane < at + n)
                target = jnp.where(held, offset - at + lane, target)
                filled[z] = at + n
                offset = offset + n
    t_ref[0:8, :] = spot
    t_ref[8:16, :] = target
    most = filled[0]
    for z in range(1, 8):
        most = jnp.maximum(most, filled[z])
    level = jnp.int32(0)
    for room in ROOMS[:-1]:
        level = level + jnp.where(most > room, 1, 0)
    level_ref[0] = level
    pltpu.make_async_copy(g_ref, o_ref, block_sem).wait()


def step_kernel(
    room,
    entries,
    o_ref,
    t_ref,
    s_ref,
    f_ref,
    scale_ref,
    a_out,
    near,
    packed,
    recv,
    acc,
    pick_ref,
    picks,
    grad,
    a,
    poly,
    root,
    moment,
    work,
    fourth,
    roots,
    ways,
    back,
    slots,
    spread_ref,
    square,
    told,
    heard,
    x_send,
    x_recv,
    z_send,
    z_recv,
    p_send,
    p_recv,
    in_sem,
    out_sem,
    root_sem,
    bz_send,
    bz_recv,
    bx_send,
    bx_recv,
    sum_send,
    sum_recv,
    loc_sem,
):
    x, z, c, y = place()
    partner = {"dp_2": (c + 1) % 2}
    y_peers = [{"mp": (y + dy) % 4} for dy in range(1, 4)]
    x_peers = [{"dp_0": (x + dx) % 4} for dx in range(1, 4)]
    barrier, count = greet(plane_peers(x, c) + z_peers(z) + y_peers)
    tiles = BLK // TILE

    def fetch(tile):
        return pltpu.make_async_copy(s_ref.at[span(tile), :], a.at[span(tile), :], in_sem.at[tile])

    def flush(tile):
        return pltpu.make_async_copy(a.at[span(tile), :], a_out.at[span(tile), :], out_sem.at[tile])

    for tile in range(tiles):
        fetch(tile).start()

    rows = lax.broadcasted_iota(jnp.int32, (256, 256), 0)
    pick_ref[...] = jnp.where(rows == t_ref[pl.ds(z, 1), :], 1.0, 0.0).astype(BF16)

    def column(line):
        turned = jnp.transpose(jnp.broadcast_to(line.astype(F32), (128, 256)))
        return jnp.concatenate([turned] * 8, axis=1)

    cols = lax.broadcasted_iota(jnp.int32, (256, BLK), 1).astype(F32)
    spread = jnp.where(column(t_ref[pl.ds(z, 1), :]) == cols, 1.0, 0.0)
    spread_ref[...] = spread[:, 0:256].astype(BF16)
    square[...] = jnp.zeros_like(square)
    pl.semaphore_wait(barrier, count)

    @pl.loop(0, 8)
    def _(step):
        tz = (z + distance(step)) % 8
        for dx in range(4):
            for dc in range(2):
                tx, tc = (x + dx) % 4, (c + dc) % 2
                if dx or dc:
                    pltpu.make_async_remote_copy(
                        o_ref.at[tx * 8 + tz, :, half_of(tc)],
                        near.at[step, slots_of(x, c), :],
                        x_send,
                        x_recv.at[step],
                        device_id={"dp_0": tx, "dp_2": tc},
                    ).start()

    @pl.loop(0, 8)
    def _(step):
        tz = (z + distance(step)) % 8
        near[step, slots_of(x, c), :] = o_ref[x * 8 + tz, :, half_of(c)]

    def pack(step):
        transfer(near.at[step, pl.ds(0, 224), :], x_send, x_recv.at[step], c).wait_recv()
        return dot(pick_ref[pl.ds(0, room), :], near[step]).astype(BF16)

    def to_partner(step):
        part = recv.at[step, :, half_of(c)]
        return pltpu.make_async_remote_copy(
            part, part, p_send.at[step], p_recv.at[step], device_id=partner
        )

    @pl.loop(0, 7)
    def _(step):
        packed[step] = pack(step)
        pltpu.make_async_remote_copy(
            packed.at[step],
            recv.at[step, :, half_of(c)],
            z_send,
            z_recv.at[step],
            device_id={"dp_1": (z + distance(step)) % 8},
        ).start()

    recv[7, :, half_of(c)] = pack(7)
    to_partner(7).start()

    @pl.loop(0, 8)
    def _(step):
        zt = (z + distance(step)) % 8
        want = column(t_ref[pl.ds(8 + zt, 1), :]) == cols
        picks[step] = jnp.where(want, 1.0, 0.0).astype(BF16)[0:room, :]

    lines = lax.broadcasted_iota(jnp.int32, (TILE, room), 0)

    def put(step, first=False, last=False):
        to_partner(step).wait_recv()
        zs = (z + 8 - distance(step)) % 8
        target = t_ref[pl.ds(8 + zs, 1), :][:, 0:room]

        @pl.loop(0, tiles)
        def _(tile):
            pick = jnp.where(lines + tile * TILE == target, 1.0, 0.0).astype(BF16)
            new = dot(pick, recv[step])
            if not first:
                new = acc[span(tile), :] + new
            if last:
                grad[span(tile), :] = new.astype(BF16)
            else:
                acc[span(tile), :] = new

    def take(step):
        transfer(packed.at[step], z_send, z_recv.at[step], c).wait_recv()
        to_partner(step).start()

    take(0)
    put(7, first=True)

    @pl.loop(1, 7)
    def _(step):
        take(step)
        put(step - 1)

    put(6, last=True)

    def gram(side):
        def add(tile, total):
            if side == 0:
                prod = dot(grad[span(tile), :], grad[...], ((1,), (1,)))
            else:
                prod = dot(grad[:, span(tile)], grad[...], ((0,), (0,)))
            new = decay_rate * a[span(tile), :] + (1.0 - decay_rate) * prod
            a[span(tile), :] = new
            return total + jnp.sum(jnp.abs(new).reshape(TILE // 8, 8, BLK), axis=0)

        work[...] = lax.fori_loop(0, tiles, add, jnp.zeros((8, BLK), F32))

    for tile in range(tiles):
        fetch(tile).wait()
    pl.when(c == 0)(lambda: gram(0))
    pl.when(c == 1)(lambda: gram(1))
    bound = jnp.max(jnp.sum(work[...], axis=0, keepdims=True), axis=1, keepdims=True)
    scale = 1.0 / bound
    factor = lax.rsqrt(jnp.sqrt(bound))
    row = lax.broadcasted_iota(jnp.int32, (TILE, BLK), 0)
    col = lax.broadcasted_iota(jnp.int32, (TILE, BLK), 1)

    def eye5(tile):
        return jnp.where(row + tile * TILE == col, 5.0, 0.0)

    @pl.loop(0, tiles)
    def _(tile):
        first = a[span(tile), :] * scale
        shifted = (eye5(tile) - first) * 0.25
        moment[span(tile), :] = first.astype(BF16)
        poly[span(tile), :] = shifted.astype(BF16)
        root[span(tile), :] = (factor * shifted).astype(BF16)

    for tile in range(tiles):
        flush(tile).start()

    @pl.loop(0, tiles)
    def _(tile):
        fourth[0, span(tile), :] = dot(poly[span(tile), :], poly[...]).astype(BF16)

    @pl.loop(0, tiles)
    def _(tile):
        fourth[1, span(tile), :] = dot(fourth[0, span(tile), :], fourth[0]).astype(BF16)

    @pl.loop(0, tiles)
    def _(tile):
        new = dot(fourth[1, span(tile), :], moment[...])
        poly[span(tile), :] = ((eye5(tile) - new) * 0.25).astype(BF16)

    @pl.loop(0, tiles)
    def _(tile):
        roots[c, span(tile), :] = dot(root[span(tile), :], poly[...]).astype(BF16)
        part = roots.at[c, span(tile), :]
        pltpu.make_async_remote_copy(
            part, part, root_sem.at[0], root_sem.at[1], device_id=partner
        ).start()

    whole = transfer(roots.at[c], root_sem.at[0], root_sem.at[1], c)
    whole.wait_recv()

    def make(step):
        picked = dot(picks[step], roots[0]).astype(BF16)
        half = dot(picked, grad[...]).astype(BF16)
        full = dot(half, roots[1, :, half_of(c)])
        ways[step] = full.astype(BF16)
        square[...] += jnp.sum((full * full).reshape(room // 8, 8, 512), axis=0)

    @pl.loop(0, 7)
    def _(step):
        make(step)
        pltpu.make_async_remote_copy(
            ways.at[step],
            back.at[step],
            bz_send,
            bz_recv.at[step],
            device_id={"dp_1": (z + distance(step)) % 8},
        ).start()

    make(7)
    one = pl.ds(0, 1)

    def tell(stage, part, peers, at):
        told[stage, one, :] = part
        for i, peer in enumerate(peers):
            pltpu.make_async_remote_copy(
                told.at[stage, one, :],
                heard.at[at + i, one, :],
                sum_send.at[stage],
                sum_recv.at[stage],
                device_id=peer,
            ).start()

    def hear(stage, part, number, at):
        ref = heard.at[pl.ds(at, number), one, :]
        transfer(ref, sum_send.at[stage], sum_recv.at[stage], c).wait()
        for i in range(number):
            part = part + heard[at + i, one, :]
        return part

    def give(step, lot):
        slots[step] = dot(spread_ref[:, 0:room], lot).astype(BF16)
        block = x * 8 + (z + 8 - distance(step)) % 8
        for dx in range(4):
            for dc in range(2):
                tx, tc = (x + dx) % 4, (c + dc) % 2
                if dx or dc:
                    pltpu.make_async_remote_copy(
                        slots.at[step, slots_of(tx, tc), :],
                        f_ref.at[block, :, half_of(c)],
                        bx_send,
                        bx_recv,
                        device_id={"dp_0": tx, "dp_2": tc},
                    ).start()
        pltpu.make_async_copy(
            slots.at[step, slots_of(x, c), :], f_ref.at[block, :, half_of(c)], loc_sem
        ).start()

    def pass_on(step):
        transfer(back.at[step], bz_send, bz_recv.at[step], c).wait_recv()
        give(step, back[step])

    own = jnp.sum(square[...], axis=0, keepdims=True)
    part = own[:, 0:128] + own[:, 128:256] + own[:, 256:384] + own[:, 384:512]
    tell(0, part, [partner], 0)
    give(7, ways[7])
    part = hear(0, part, 1, 0)
    tell(1, part, y_peers, 1)
    pass_on(0)
    part = hear(1, part, 3, 1)
    tell(2, part, x_peers, 4)
    pass_on(1)
    part = hear(2, part, 3, 4)
    tell(3, part, z_peers(z), 7)

    @pl.loop(2, 7)
    def _(step):
        pass_on(step)

    part = hear(3, part, 7, 7)
    mean = jnp.sum(part, axis=1, keepdims=True) * (1.0 / entries)
    scale_ref[...] = jnp.broadcast_to(lax.rsqrt(mean + epsilon), (8, 128))

    @pl.loop(0, 8)
    def _(step):
        to_partner(step).wait_send()

    transfer(near.at[pl.ds(0, 7)], x_send, x_recv.at[0], c).wait_send()
    transfer(packed, z_send, z_recv.at[0], c).wait_send()
    whole.wait_send()
    for tile in range(tiles):
        flush(tile).wait()
    transfer(ways.at[pl.ds(0, 7)], bz_send, bz_recv.at[0], c).wait_send()
    transfer(slots.at[pl.ds(0, 7)], bx_send, bx_recv, c).wait_send()
    pltpu.make_async_copy(slots.at[0], slots.at[0], loc_sem).wait()
    transfer(f_ref.at[pl.ds(0, 28)], bx_send, bx_recv, c).wait_recv()


def finish_kernel(
    pair_ref, scale_ref, f_ref, a_ref, u_ref, a_out, pair, block, held, a, sem, in_sem, out_sem, u_sem
):
    first = pltpu.make_async_copy(pair_ref, pair, sem.at[0])
    second = pltpu.make_async_copy(f_ref, block, sem.at[1])
    first.start()
    second.start()

    def fetch(tile):
        return pltpu.make_async_copy(a_ref.at[span(tile), :], a.at[span(tile), :], in_sem.at[tile])

    def store(tile):
        return pltpu.make_async_copy(a.at[span(tile), :], a_out.at[span(tile), :], out_sem.at[tile])

    def flush(group):
        part = pl.ds(group * 8, 8)
        return pltpu.make_async_copy(held.at[part], u_ref.at[part], u_sem.at[group])

    for tile in range(4):
        fetch(tile).start()
    scale = scale_ref[0:1, 0:1]
    first.wait()
    second.wait()

    @pl.loop(0, 4)
    def _(group):
        for i in range(8):
            k = group * 8 + i
            held[k] = (block[pair[k]].astype(F32) * scale).astype(BF16)
        flush(group).start()
        fetch(group).wait()
        store(group).start()

    for group in range(4):
        flush(group).wait()
        store(group).wait()


VMEM = pl.BlockSpec(memory_space=pltpu.VMEM)
SMEM = pl.BlockSpec(memory_space=pltpu.SMEM)
HBM = pl.BlockSpec(memory_space=pltpu.HBM)
DMA = pltpu.SemaphoreType.DMA
ROOMS = (176, 192, 208, 256)


def shape(dims, kind):
    return jax.ShapeDtypeStruct(dims, kind)


def step_call(room, number, entries):
    return pl.pallas_call(
        functools.partial(step_kernel, room, entries),
        out_shape=(
            shape((32, 32, BLK), BF16),
            shape((8, 128), F32),
            shape((BLK, BLK), F32),
        ),
        in_specs=[VMEM, VMEM, HBM],
        out_specs=(HBM, VMEM, HBM),
        scratch_shapes=[
            pltpu.VMEM((8, 256, 512), BF16),
            pltpu.VMEM((7, room, 512), BF16),
            pltpu.VMEM((8, room, BLK), BF16),
            pltpu.VMEM((BLK, BLK), F32),
            pltpu.VMEM((256, 256), BF16),
            pltpu.VMEM((8, room, BLK), BF16),
            pltpu.VMEM((BLK, BLK), BF16),
            pltpu.VMEM((BLK, BLK), F32),
            pltpu.VMEM((BLK, BLK), BF16),
            pltpu.VMEM((BLK, BLK), BF16),
            pltpu.VMEM((BLK, BLK), BF16),
            pltpu.VMEM((8, BLK), F32),
            pltpu.VMEM((2, BLK, BLK), BF16),
            pltpu.VMEM((2, BLK, BLK), BF16),
            pltpu.VMEM((8, room, 512), BF16),
            pltpu.VMEM((7, room, 512), BF16),
            pltpu.VMEM((8, 256, 512), BF16),
            pltpu.VMEM((256, 256), BF16),
            pltpu.VMEM((8, 512), F32),
            pltpu.VMEM((4, 8, 128), F32),
            pltpu.VMEM((16, 8, 128), F32),
            DMA,
            DMA((8,)),
            DMA,
            DMA((7,)),
            DMA((8,)),
            DMA((8,)),
            DMA((4,)),
            DMA((4,)),
            DMA((2,)),
            DMA,
            DMA((7,)),
            DMA,
            DMA,
            DMA((4,)),
            DMA((4,)),
            DMA,
        ],
        compiler_params=pltpu.CompilerParams(
            collective_id=number, has_side_effects=True, vmem_limit_bytes=56 << 20
        ),
        name=f"step_{room}",
    )


def body(gradients, statistics, row_counts, block_pair):
    blocks = gradients.shape[0]
    outgoing, table, level = pl.pallas_call(
        deal_kernel,
        out_shape=(
            shape(gradients.shape, BF16),
            shape((16, 256), jnp.int32),
            shape((1,), jnp.int32),
        ),
        in_specs=[HBM, HBM, HBM],
        out_specs=(VMEM, VMEM, SMEM),
        scratch_shapes=[
            pltpu.SMEM((64,), jnp.int32),
            pltpu.SMEM((32,), jnp.int32),
            DMA((2,)),
            DMA,
        ],
        compiler_params=pltpu.CompilerParams(vmem_limit_bytes=64900000),
        name="deal",
    )(row_counts, block_pair, gradients)

    entries = lax.axis_size("mp") * blocks * BLK * BLK
    returned, scale, accumulated = lax.switch(
        level[0],
        [step_call(room, i, entries) for i, room in enumerate(ROOMS)],
        outgoing,
        table,
        statistics,
    )

    return pl.pallas_call(
        finish_kernel,
        out_shape=(shape(gradients.shape, BF16), shape((BLK, BLK), F32)),
        in_specs=[HBM, VMEM, HBM, HBM],
        out_specs=(HBM, HBM),
        scratch_shapes=[
            pltpu.SMEM((32,), jnp.int32),
            pltpu.VMEM(gradients.shape, BF16),
            pltpu.VMEM(gradients.shape, BF16),
            pltpu.VMEM((BLK, BLK), F32),
            DMA((2,)),
            DMA((4,)),
            DMA((4,)),
            DMA((4,)),
        ],
        compiler_params=pltpu.CompilerParams(vmem_limit_bytes=24 << 20),
        name="finish",
    )(block_pair, scale, returned, accumulated)


def solution(mesh):
    torus = Mesh(mesh.devices.reshape(4, 8, 2, mesh.shape["mp"]), DP + ("mp",))
    placed = (P(None, DP, "mp"), P(DP, "mp"), P(), P())
    return jax.shard_map(
        body,
        mesh=torus,
        in_specs=placed,
        out_specs=(P(None, DP, "mp"), P(DP, "mp")),
        check_vma=False,
    )
```

```python
import functools

import jax
import jax.numpy as jnp
from jax import lax
from jax.experimental import pallas as pl
from jax.experimental.pallas import tpu as pltpu
from jax.sharding import Mesh
from jax.sharding import PartitionSpec as P

DP = ("dp_0", "dp_1", "dp_2")
BLK = 1024
TILE = 256
F32 = jnp.float32
BF16 = jnp.bfloat16

decay_rate = 0.95
epsilon = 1e-06


def place():
    return (
        lax.axis_index("dp_0"),
        lax.axis_index("dp_1"),
        lax.axis_index("dp_2"),
        lax.axis_index("mp"),
    )


def distance(step):
    odd = step % 2
    return (4 + odd * ((step + 1) // 2) - (1 - odd) * (step // 2)) % 8


def outward(step):
    if isinstance(step, int) and step == 7:
        return 0
    odd = step % 2
    return (1 - odd) * (1 + step // 2) + odd * (7 - step // 2)


def dot(a, b, dims=((1,), (0,))):
    return lax.dot_general(a, b, (dims, ((), ())), preferred_element_type=F32)


def greet(peers):
    barrier = pltpu.get_barrier_semaphore()
    for peer in peers:
        pl.semaphore_signal(barrier, inc=1, device_id=peer)
    return barrier, len(peers)


def plane_peers(x, c):
    return [
        {"dp_0": (x + dx) % 4, "dp_2": (c + dc) % 2}
        for dx in range(4)
        for dc in range(2)
        if dx or dc
    ]


def z_peers(z):
    return [{"dp_1": (z + dz) % 8} for dz in range(1, 8)]


def transfer(ref, send_sem, recv_sem, c):
    return pltpu.make_async_remote_copy(
        ref, ref, send_sem, recv_sem, device_id={"dp_2": (c + 1) % 2}
    )


def half_of(c):
    return pl.ds(pl.multiple_of(512 * c, 512), 512)


def slots_of(x, c):
    return pl.ds(pl.multiple_of(32 * (2 * x + c), 32), 32)


def span(tile):
    return pl.ds(pl.multiple_of(tile * TILE, TILE), TILE)


def deal_kernel(
    counts_ref, pair_ref, g_ref, o_ref, t_ref, level_ref, counts, pair, sem, block_sem
):
    first = pltpu.make_async_copy(pair_ref, pair, sem.at[0])
    second = pltpu.make_async_copy(counts_ref, counts, sem.at[1])
    first.start()
    second.start()
    first.wait()

    @pl.loop(0, 32)
    def _(k):
        pltpu.make_async_copy(g_ref.at[k], o_ref.at[pair[k]], block_sem).start()

    second.wait()
    lane = lax.broadcasted_iota(jnp.int32, (8, 256), 1)
    plane = lax.broadcasted_iota(jnp.int32, (8, 256), 0)
    inner = lane % 32
    group = lane // 32
    spot = jnp.full((8, 256), -1, jnp.int32)
    target = jnp.full((8, 256), -1, jnp.int32)
    offset = counts[0] * 0
    filled = [offset] * 8
    for x in range(4):
        for z in range(8):
            for c in range(2):
                q = (x * 8 + z) * 2 + c
                n = counts[q]
                at = filled[z]
                here = (plane == z) & (group == 2 * x + c) & (inner < n)
                spot = jnp.where(here, at + inner, spot)
                held = (plane == z) & (lane >= at) & (lane < at + n)
                target = jnp.where(held, offset - at + lane, target)
                filled[z] = at + n
                offset = offset + n
    t_ref[0:8, :] = spot
    t_ref[8:16, :] = target
    most = filled[0]
    for z in range(1, 8):
        most = jnp.maximum(most, filled[z])
    level = jnp.int32(0)
    for room in ROOMS[:-1]:
        level = level + jnp.where(most > room, 1, 0)
    level_ref[0] = level
    pltpu.make_async_copy(g_ref, o_ref, block_sem).wait()


def step_kernel(
    room,
    entries,
    o_ref,
    t_ref,
    s_ref,
    f_ref,
    scale_ref,
    a_out,
    near,
    packed,
    recv,
    acc,
    pick_ref,
    picks,
    grad,
    a,
    poly,
    root,
    moment,
    work,
    fourth,
    roots,
    ways,
    back,
    slots,
    spread_ref,
    square,
    told,
    heard,
    x_send,
    x_recv,
    z_send,
    z_recv,
    p_send,
    p_recv,
    in_sem,
    out_sem,
    root_sem,
    bz_send,
    bz_recv,
    bx_send,
    bx_recv,
    sum_send,
    sum_recv,
    loc_sem,
):
    x, z, c, y = place()
    partner = {"dp_2": (c + 1) % 2}
    y_peers = [{"mp": (y + dy) % 4} for dy in range(1, 4)]
    x_peers = [{"dp_0": (x + dx) % 4} for dx in range(1, 4)]
    barrier, count = greet(plane_peers(x, c) + z_peers(z) + y_peers)
    tiles = BLK // TILE

    def fetch(tile):
        return pltpu.make_async_copy(s_ref.at[span(tile), :], a.at[span(tile), :], in_sem.at[tile])

    def flush(tile):
        return pltpu.make_async_copy(a.at[span(tile), :], a_out.at[span(tile), :], out_sem.at[tile])

    for tile in range(tiles):
        fetch(tile).start()

    rows = lax.broadcasted_iota(jnp.int32, (256, 256), 0)
    pick_ref[...] = jnp.where(rows == t_ref[pl.ds(z, 1), :], 1.0, 0.0).astype(BF16)

    def column(line):
        turned = jnp.transpose(jnp.broadcast_to(line.astype(F32), (128, 256)))
        return jnp.concatenate([turned] * 8, axis=1)

    cols = lax.broadcasted_iota(jnp.int32, (256, BLK), 1).astype(F32)
    spread = jnp.where(column(t_ref[pl.ds(z, 1), :]) == cols, 1.0, 0.0)
    spread_ref[...] = spread[:, 0:256].astype(BF16)
    square[...] = jnp.zeros_like(square)
    pl.semaphore_wait(barrier, count)

    @pl.loop(0, 8)
    def _(step):
        tz = (z + distance(step)) % 8
        for dx in range(4):
            for dc in range(2):
                tx, tc = (x + dx) % 4, (c + dc) % 2
                if dx or dc:
                    pltpu.make_async_remote_copy(
                        o_ref.at[tx * 8 + tz, :, half_of(tc)],
                        near.at[step, slots_of(x, c), :],
                        x_send,
                        x_recv.at[step],
                        device_id={"dp_0": tx, "dp_2": tc},
                    ).start()

    @pl.loop(0, 8)
    def _(step):
        tz = (z + distance(step)) % 8
        near[step, slots_of(x, c), :] = o_ref[x * 8 + tz, :, half_of(c)]

    def pack(step):
        transfer(near.at[step, pl.ds(0, 224), :], x_send, x_recv.at[step], c).wait_recv()
        return dot(pick_ref[pl.ds(0, room), :], near[step]).astype(BF16)

    def to_partner(step):
        part = recv.at[step, :, half_of(c)]
        return pltpu.make_async_remote_copy(
            part, part, p_send.at[step], p_recv.at[step], device_id=partner
        )

    def choose(step):
        zt = (z + outward(step)) % 8
        want = column(t_ref[pl.ds(8 + zt, 1), :]) == cols
        picks[step] = jnp.where(want, 1.0, 0.0).astype(BF16)[0:room, :]

    choose(7)

    @pl.loop(0, 7)
    def _(step):
        packed[step] = pack(step)
        pltpu.make_async_remote_copy(
            packed.at[step],
            recv.at[step, :, half_of(c)],
            z_send,
            z_recv.at[step],
            device_id={"dp_1": (z + distance(step)) % 8},
        ).start()
        choose(step)

    recv[7, :, half_of(c)] = pack(7)
    to_partner(7).start()

    lines = lax.broadcasted_iota(jnp.int32, (TILE, room), 0)

    def put(step, first=False, last=False):
        to_partner(step).wait_recv()
        zs = (z + 8 - distance(step)) % 8
        target = t_ref[pl.ds(8 + zs, 1), :][:, 0:room]

        @pl.loop(0, tiles)
        def _(tile):
            pick = jnp.where(lines + tile * TILE == target, 1.0, 0.0).astype(BF16)
            new = dot(pick, recv[step])
            if not first:
                new = acc[span(tile), :] + new
            if last:
                grad[span(tile), :] = new.astype(BF16)
            else:
                acc[span(tile), :] = new

    def take(step):
        transfer(packed.at[step], z_send, z_recv.at[step], c).wait_recv()
        to_partner(step).start()

    take(0)
    put(7, first=True)

    @pl.loop(1, 7)
    def _(step):
        take(step)
        put(step - 1)

    put(6, last=True)

    def gram(side):
        def add(tile, total):
            if side == 0:
                prod = dot(grad[span(tile), :], grad[...], ((1,), (1,)))
            else:
                prod = dot(grad[:, span(tile)], grad[...], ((0,), (0,)))
            new = decay_rate * a[span(tile), :] + (1.0 - decay_rate) * prod
            a[span(tile), :] = new
            return total + jnp.sum(jnp.abs(new).reshape(TILE // 8, 8, BLK), axis=0)

        work[...] = lax.fori_loop(0, tiles, add, jnp.zeros((8, BLK), F32))

    for tile in range(tiles):
        fetch(tile).wait()
    pl.when(c == 0)(lambda: gram(0))
    pl.when(c == 1)(lambda: gram(1))
    bound = jnp.max(jnp.sum(work[...], axis=0, keepdims=True), axis=1, keepdims=True)
    scale = 1.0 / bound
    factor = lax.rsqrt(jnp.sqrt(bound))
    row = lax.broadcasted_iota(jnp.int32, (TILE, BLK), 0)
    col = lax.broadcasted_iota(jnp.int32, (TILE, BLK), 1)

    def eye5(tile):
        return jnp.where(row + tile * TILE == col, 5.0, 0.0)

    @pl.loop(0, tiles)
    def _(tile):
        first = a[span(tile), :] * scale
        shifted = (eye5(tile) - first) * 0.25
        moment[span(tile), :] = first.astype(BF16)
        poly[span(tile), :] = shifted.astype(BF16)
        root[span(tile), :] = (factor * shifted).astype(BF16)

    for tile in range(tiles):
        flush(tile).start()

    @pl.loop(0, tiles)
    def _(tile):
        fourth[0, span(tile), :] = dot(poly[span(tile), :], poly[...]).astype(BF16)

    @pl.loop(0, tiles)
    def _(tile):
        fourth[1, span(tile), :] = dot(fourth[0, span(tile), :], fourth[0]).astype(BF16)

    @pl.loop(0, tiles)
    def _(tile):
        new = dot(fourth[1, span(tile), :], moment[...])
        poly[span(tile), :] = ((eye5(tile) - new) * 0.25).astype(BF16)

    @pl.loop(0, tiles)
    def _(tile):
        roots[c, span(tile), :] = dot(root[span(tile), :], poly[...]).astype(BF16)
        part = roots.at[c, span(tile), :]
        pltpu.make_async_remote_copy(
            part, part, root_sem.at[0], root_sem.at[1], device_id=partner
        ).start()

    whole = transfer(roots.at[c], root_sem.at[0], root_sem.at[1], c)
    whole.wait_recv()

    def make(step):
        picked = dot(picks[step], roots[0]).astype(BF16)
        half = dot(picked, grad[...]).astype(BF16)
        full = dot(half, roots[1, :, half_of(c)])
        ways[step] = full.astype(BF16)
        square[...] += jnp.sum((full * full).reshape(room // 8, 8, 512), axis=0)

    @pl.loop(0, 7)
    def _(step):
        make(step)
        pltpu.make_async_remote_copy(
            ways.at[step],
            back.at[step],
            bz_send,
            bz_recv.at[step],
            device_id={"dp_1": (z + outward(step)) % 8},
        ).start()

    make(7)
    one = pl.ds(0, 1)

    def tell(stage, part, peers, at):
        told[stage, one, :] = part
        for i, peer in enumerate(peers):
            pltpu.make_async_remote_copy(
                told.at[stage, one, :],
                heard.at[at + i, one, :],
                sum_send.at[stage],
                sum_recv.at[stage],
                device_id=peer,
            ).start()

    def hear(stage, part, number, at):
        ref = heard.at[pl.ds(at, number), one, :]
        transfer(ref, sum_send.at[stage], sum_recv.at[stage], c).wait()
        for i in range(number):
            part = part + heard[at + i, one, :]
        return part

    def give(step, lot):
        slots[step] = dot(spread_ref[:, 0:room], lot).astype(BF16)
        block = x * 8 + (z + 8 - outward(step)) % 8
        for dx in range(4):
            for dc in range(2):
                tx, tc = (x + dx) % 4, (c + dc) % 2
                if dx or dc:
                    pltpu.make_async_remote_copy(
                        slots.at[step, slots_of(tx, tc), :],
                        f_ref.at[block, :, half_of(c)],
                        bx_send,
                        bx_recv,
                        device_id={"dp_0": tx, "dp_2": tc},
                    ).start()
        pltpu.make_async_copy(
            slots.at[step, slots_of(x, c), :], f_ref.at[block, :, half_of(c)], loc_sem
        ).start()

    def pass_on(step):
        transfer(back.at[step], bz_send, bz_recv.at[step], c).wait_recv()
        give(step, back[step])

    own = jnp.sum(square[...], axis=0, keepdims=True)
    part = own[:, 0:128] + own[:, 128:256] + own[:, 256:384] + own[:, 384:512]
    tell(0, part, [partner], 0)
    give(7, ways[7])
    part = hear(0, part, 1, 0)
    tell(1, part, y_peers, 1)
    pass_on(0)
    part = hear(1, part, 3, 1)
    tell(2, part, x_peers, 4)
    pass_on(1)
    part = hear(2, part, 3, 4)
    tell(3, part, z_peers(z), 7)

    @pl.loop(2, 7)
    def _(step):
        pass_on(step)

    part = hear(3, part, 7, 7)
    mean = jnp.sum(part, axis=1, keepdims=True) * (1.0 / entries)
    scale_ref[...] = jnp.broadcast_to(lax.rsqrt(mean + epsilon), (8, 128))

    @pl.loop(0, 8)
    def _(step):
        to_partner(step).wait_send()

    transfer(near.at[pl.ds(0, 7)], x_send, x_recv.at[0], c).wait_send()
    transfer(packed, z_send, z_recv.at[0], c).wait_send()
    whole.wait_send()
    for tile in range(tiles):
        flush(tile).wait()
    transfer(ways.at[pl.ds(0, 7)], bz_send, bz_recv.at[0], c).wait_send()
    transfer(slots.at[pl.ds(0, 7)], bx_send, bx_recv, c).wait_send()
    pltpu.make_async_copy(slots.at[0], slots.at[0], loc_sem).wait()
    transfer(f_ref.at[pl.ds(0, 28)], bx_send, bx_recv, c).wait_recv()


def finish_kernel(
    pair_ref, scale_ref, f_ref, a_ref, u_ref, a_out, pair, block, held, a, sem, in_sem, out_sem, u_sem
):
    first = pltpu.make_async_copy(pair_ref, pair, sem.at[0])
    second = pltpu.make_async_copy(f_ref, block, sem.at[1])
    first.start()
    second.start()

    def fetch(tile):
        return pltpu.make_async_copy(a_ref.at[span(tile), :], a.at[span(tile), :], in_sem.at[tile])

    def store(tile):
        return pltpu.make_async_copy(a.at[span(tile), :], a_out.at[span(tile), :], out_sem.at[tile])

    def flush(group):
        part = pl.ds(group * 8, 8)
        return pltpu.make_async_copy(held.at[part], u_ref.at[part], u_sem.at[group])

    for tile in range(4):
        fetch(tile).start()
    scale = scale_ref[0:1, 0:1]
    first.wait()
    second.wait()

    @pl.loop(0, 4)
    def _(group):
        for i in range(8):
            k = group * 8 + i
            held[k] = (block[pair[k]].astype(F32) * scale).astype(BF16)
        flush(group).start()
        fetch(group).wait()
        store(group).start()

    for group in range(4):
        flush(group).wait()
        store(group).wait()


VMEM = pl.BlockSpec(memory_space=pltpu.VMEM)
SMEM = pl.BlockSpec(memory_space=pltpu.SMEM)
HBM = pl.BlockSpec(memory_space=pltpu.HBM)
DMA = pltpu.SemaphoreType.DMA
ROOMS = (176, 192, 208, 256)


def shape(dims, kind):
    return jax.ShapeDtypeStruct(dims, kind)


def step_call(room, number, entries):
    return pl.pallas_call(
        functools.partial(step_kernel, room, entries),
        out_shape=(
            shape((32, 32, BLK), BF16),
            shape((8, 128), F32),
            shape((BLK, BLK), F32),
        ),
        in_specs=[VMEM, VMEM, HBM],
        out_specs=(HBM, VMEM, HBM),
        scratch_shapes=[
            pltpu.VMEM((8, 256, 512), BF16),
            pltpu.VMEM((7, room, 512), BF16),
            pltpu.VMEM((8, room, BLK), BF16),
            pltpu.VMEM((BLK, BLK), F32),
            pltpu.VMEM((256, 256), BF16),
            pltpu.VMEM((8, room, BLK), BF16),
            pltpu.VMEM((BLK, BLK), BF16),
            pltpu.VMEM((BLK, BLK), F32),
            pltpu.VMEM((BLK, BLK), BF16),
            pltpu.VMEM((BLK, BLK), BF16),
            pltpu.VMEM((BLK, BLK), BF16),
            pltpu.VMEM((8, BLK), F32),
            pltpu.VMEM((2, BLK, BLK), BF16),
            pltpu.VMEM((2, BLK, BLK), BF16),
            pltpu.VMEM((8, room, 512), BF16),
            pltpu.VMEM((7, room, 512), BF16),
            pltpu.VMEM((8, 256, 512), BF16),
            pltpu.VMEM((256, 256), BF16),
            pltpu.VMEM((8, 512), F32),
            pltpu.VMEM((4, 8, 128), F32),
            pltpu.VMEM((16, 8, 128), F32),
            DMA,
            DMA((8,)),
            DMA,
            DMA((7,)),
            DMA((8,)),
            DMA((8,)),
            DMA((4,)),
            DMA((4,)),
            DMA((2,)),
            DMA,
            DMA((7,)),
            DMA,
            DMA,
            DMA((4,)),
            DMA((4,)),
            DMA,
        ],
        compiler_params=pltpu.CompilerParams(
            collective_id=number, has_side_effects=True, vmem_limit_bytes=56 << 20
        ),
        name=f"step_{room}",
    )


def body(gradients, statistics, row_counts, block_pair):
    blocks = gradients.shape[0]
    outgoing, table, level = pl.pallas_call(
        deal_kernel,
        out_shape=(
            shape(gradients.shape, BF16),
            shape((16, 256), jnp.int32),
            shape((1,), jnp.int32),
        ),
        in_specs=[HBM, HBM, HBM],
        out_specs=(VMEM, VMEM, SMEM),
        scratch_shapes=[
            pltpu.SMEM((64,), jnp.int32),
            pltpu.SMEM((32,), jnp.int32),
            DMA((2,)),
            DMA,
        ],
        compiler_params=pltpu.CompilerParams(vmem_limit_bytes=64900000),
        name="deal",
    )(row_counts, block_pair, gradients)

    entries = lax.axis_size("mp") * blocks * BLK * BLK
    returned, scale, accumulated = lax.switch(
        level[0],
        [step_call(room, i, entries) for i, room in enumerate(ROOMS)],
        outgoing,
        table,
        statistics,
    )

    return pl.pallas_call(
        finish_kernel,
        out_shape=(shape(gradients.shape, BF16), shape((BLK, BLK), F32)),
        in_specs=[HBM, VMEM, HBM, HBM],
        out_specs=(HBM, HBM),
        scratch_shapes=[
            pltpu.SMEM((32,), jnp.int32),
            pltpu.VMEM(gradients.shape, BF16),
            pltpu.VMEM(gradients.shape, BF16),
            pltpu.VMEM((BLK, BLK), F32),
            DMA((2,)),
            DMA((4,)),
            DMA((4,)),
            DMA((4,)),
        ],
        compiler_params=pltpu.CompilerParams(vmem_limit_bytes=24 << 20),
        name="finish",
    )(block_pair, scale, returned, accumulated)


def solution(mesh):
    torus = Mesh(mesh.devices.reshape(4, 8, 2, mesh.shape["mp"]), DP + ("mp",))
    placed = (P(None, DP, "mp"), P(DP, "mp"), P(), P())
    return jax.shard_map(
        body,
        mesh=torus,
        in_specs=placed,
        out_specs=(P(None, DP, "mp"), P(DP, "mp")),
        check_vma=False,
    )
```
